32 devices in a mesh: groups: 2 (over y), dp: 4 (over z), tensor: 4 (over x, core).
Axes of the slice: x: 2, y: 2, z: 4, core: 2. Of those that a mesh axis runs over, the one named last changes fastest.
Arguments:
- tokens: bfloat16 [4096, 4096], P(('groups', 'dp')), parts along dimension 0, may hold values from -6 to 6
- w_query: bfloat16 [4096, 4096], P('dp', 'tensor'), may hold values from -0.09375 to 0.09375
- w_key: bfloat16 [4096, 1024], P('dp', 'tensor'), may hold values from -0.09375 to 0.09375
- w_value: bfloat16 [4096, 1024], P('dp', 'tensor'), may hold values from -0.09375 to 0.09375
- a_query: bfloat16 [8, 4096, 32], P(('groups', 'dp'), 'tensor'), parts along dimension 0, may hold values from -0.09375 to 0.09375
- b_query: bfloat16 [8, 32, 4096], P(('groups', 'dp'), None, 'tensor'), parts along dimension 0, may hold values from -1 to 1
- a_value: bfloat16 [8, 4096, 32], P(('groups', 'dp'), 'tensor'), parts along dimension 0, may hold values from -0.09375 to 0.09375
- b_value: bfloat16 [8, 32, 1024], P(('groups', 'dp'), None, 'tensor'), parts along dimension 0, may hold values from -1 to 1
- adapter_ranks: int32 [8], P('groups'), parts along dimension 0, may hold values from 16 to 32
- adapter_slot: int32 [4], replicated, may hold values from 0 to 3, each once
- block_adapter: int32 [32, 1], P(('groups', 'dp')), parts along dimension 0, may hold values from 0 to 3
- live_tokens: int32 [8], P(('groups', 'dp')), parts along dimension 0, may hold values from 1 to 512, 1280 in all
- d_heads: bfloat16 [4096, 4096], P(('groups', 'dp'), 'tensor'), parts along dimension 0, may hold values from -0.29882812 to 0.29882812
Outputs:
- grad_a_query: float32 [8, 4096, 32], P(('groups', 'dp'), 'tensor'), parts along dimension 0
- grad_b_query: float32 [8, 32, 4096], P(('groups', 'dp'), None, 'tensor'), parts along dimension 0
- grad_a_value: float32 [8, 4096, 32], P(('groups', 'dp'), 'tensor'), parts along dimension 0
- grad_b_value: float32 [8, 32, 1024], P(('groups', 'dp'), None, 'tensor'), parts along dimension 0
The draws below stay inside these ranges and needn't reach their ends.
There are 2 independent parts, one for each index of `groups`. The reference program is written for one: setup_inputs(seed, part) draws one part's arguments, and reference() takes and returns one part's arrays. A program takes and returns all parts, laid end to end along the dimension named above; an argument that names none is the same for every part. Nothing has to cross between parts.
Inputs may be any that keep to these rules, and one draw needn't show every extreme that they name: `adapter_slot`: each slot holds exactly one adapter. `block_adapter`: every adapter is named by some block. `live_tokens`: one index of dp has all its rows live.
All inputs are finite; a program needn't handle non-finite values. No bound on the sum of `live_tokens` on one device may be relied on, other than what follows from the above.
Results may differ from the reference program's by a relative error of at most 0.02.
Values may be sent and summed in bfloat16 or wider, within the bound.
A program may use at most 64 MiB of HBM per device.

```python
import math
import jax
import jax.numpy as jnp
import numpy as np
from jax import lax

D = 4096
HEADS = 32
KVH = 8
HD = 128
R = 32
REQUEST_ROWS = 128
BLOCKS_DEV = 4
TOK_DEV = 512
TOKENS = 2048
ADAPTERS = 4
N_DP = 4


def touch_ends(result, rng, low, top_value):
    index_at = [jax.random.randint(jax.random.fold_in(rng, axis), (), 0, length) for axis, length in enumerate(result.shape)]
    widest = result.shape.index(max(result.shape))
    next_to = index_at[:widest] + [(index_at[widest] + 1) % result.shape[widest]] + index_at[widest + 1:]
    return result.at[tuple(index_at)].set(low).at[tuple(next_to)].set(top_value)


def block_scale(key, extent, pieces, low, top_value):
    def one(dim, blocks):
        steps = jax.random.uniform(jax.random.fold_in(jax.random.fold_in(key, 6), dim), (blocks,), jnp.float32, low / len(pieces), top_value / len(pieces))
        return jnp.repeat(jnp.exp(steps), extent[dim] // blocks).reshape((-1,) + (1,) * (len(extent) - dim - 1))

    gain = one(*pieces[0])
    for cut in pieces[1:]:
        gain = gain * one(*cut)
    return gain


def distinct(own_key, rows, number_of, top, lift):
    sequence = jax.random.permutation(jax.random.fold_in(own_key, 1), number_of)
    boost = sequence
    for power in range(3):
        boost = boost * boost // number_of
    boost = boost * lift // number_of
    chance = jax.random.randint(jax.random.fold_in(own_key, 2), (rows, number_of), 0, 4096) + boost
    sure = jax.random.permutation(jax.random.fold_in(own_key, 3), rows)[jnp.arange(number_of) % rows]
    chance = jnp.where(jnp.arange(rows)[:, None] == sure[None, :], 1 << 14, chance)
    priority = chance * number_of + jnp.arange(number_of)
    return lax.top_k(priority.astype(jnp.int32), top)[1].astype(jnp.int32)


def split_up(number_of, total, bound, skew):
    portions = [(1 << 20) // math.isqrt(grade ** skew) + 1 for grade in range(2, number_of + 1)]
    surplus, given = total - bound - (number_of - 1), [1] * (number_of - 1)
    while surplus > 0:
        free = [i for i in range(number_of - 1) if given[i] < bound]
        pool, budget = sum([portions[i] for i in free]), surplus
        for i in free:
            more = min(bound - given[i], max(1, budget * portions[i] // pool), surplus)
            given[i] = given[i] + more
            surplus = surplus - more
    return np.array([bound] + given)


def uneven(own_key, number_of, total, bound, skew):
    if number_of == 2:
        one = jax.random.randint(own_key, (), max(1, total - bound), min(bound, total - 1) + 1)
        return jnp.stack([one, total - one])
    lengths = jnp.asarray(split_up(number_of, total, bound, skew), jnp.int32)
    pairs = (number_of - 1) // 2
    source_of, receiver = lengths[1:1 + 2 * pairs:2], lengths[2:2 + 2 * pairs:2]
    slack = jnp.minimum(source_of - 1, bound - receiver)
    passed = jax.random.randint(jax.random.fold_in(own_key, 1), (pairs,), 0, 1 << 20) % (slack + 1)
    lengths = lengths.at[1:1 + 2 * pairs:2].set(source_of - passed).at[2:2 + 2 * pairs:2].set(receiver + passed)
    return lengths[jax.random.permutation(jax.random.fold_in(own_key, 2), number_of)]


def centred(rng, dims, scale, bound, split=(), kind=jnp.bfloat16):
    array = jax.random.normal(rng, dims, jnp.float32) * scale
    if len(split) > 0:
        array = block_scale(rng, dims, split, -0.22, 0.18) * array
    return jnp.clip(array, min=-bound, max=bound).astype(kind)


def setup_inputs(seed: int = 0, part: int = 0) -> dict:
    arg_keys = jax.random.split(jax.random.key(seed), 14)
    part_splits = jax.random.split(jax.random.fold_in(arg_keys[13], part), 14)
    tokens = centred(part_splits[0], (TOKENS, D), 1.0, 6.0, ((0, 4),))
    w_query = centred(arg_keys[1], (D, HEADS * HD), D ** -0.5, 0.09375, ((0, 4), (1, 4)))
    w_key = centred(arg_keys[2], (D, KVH * HD), D ** -0.5, 0.09375, ((0, 4), (1, 4)))
    w_value = centred(arg_keys[3], (D, KVH * HD), D ** -0.5, 0.09375, ((0, 4), (1, 4)))
    a_query = centred(part_splits[4], (ADAPTERS, D, R), D ** -0.5, 0.09375, ((0, 4), (1, 4)))
    b_query = centred(part_splits[5], (ADAPTERS, R, HEADS * HD), R ** -0.5, 1.0, ((0, 4), (2, 4)))
    a_value = centred(part_splits[6], (ADAPTERS, D, R), D ** -0.5, 0.09375, ((0, 4), (1, 4)))
    b_value = centred(part_splits[7], (ADAPTERS, R, KVH * HD), R ** -0.5, 1.0, ((0, 4), (2, 4)))
    adapter_ranks = touch_ends(jax.random.randint(part_splits[8], (ADAPTERS,), R // 2, R + 1), jax.random.fold_in(part_splits[8], 1), R // 2, R).astype(jnp.int32)
    adapter_slot = jax.random.permutation(arg_keys[9], ADAPTERS).astype(jnp.int32)
    block_adapter = distinct(part_splits[10], (TOKENS // REQUEST_ROWS), ADAPTERS, 1, 4096)
    live_tokens = uneven(part_splits[11], N_DP, N_DP * TOK_DEV * 5 // 8, TOK_DEV, 2).astype(jnp.int32)
    d_heads = centred(part_splits[12], (TOKENS, HEADS * HD), 0.05, 0.29882812, ((0, 4), (1, 4)))
    return {"tokens": tokens, "w_query": w_query, "w_key": w_key, "w_value": w_value, "a_query": a_query, "b_query": b_query, "a_value": a_value, "b_value": b_value, "adapter_ranks": adapter_ranks, "adapter_slot": adapter_slot, "block_adapter": block_adapter, "live_tokens": live_tokens, "d_heads": d_heads}


adapter_alpha_factor = 32.0
rope_theta = 500000.0


def rope_tables(length, width):
    halfway = width // 2
    spread = rope_theta ** (-2.0 * jnp.arange(halfway, dtype=jnp.float32) / width)
    angle = jnp.arange(length, dtype=jnp.float32)[:, None] * spread[None, :]
    return jnp.cos(angle), jnp.sin(angle)


def rotate(value_matrix, cosine, sine):
    halfway = value_matrix.shape[-1] // 2
    first = value_matrix[..., :halfway]
    second = value_matrix[..., halfway:]
    cos_grid = cosine[:, None, :]
    sin_grid = sine[:, None, :]
    return jnp.concatenate([first * cos_grid - second * sin_grid, second * cos_grid + first * sin_grid], axis=-1)


def attention_grads(queries, keys, value_matrix, dout, allowed, group):
    request_block_count, length, heads, depth = queries.shape
    kv_heads = keys.shape[2]
    grouped_q = queries.reshape(request_block_count, length, kv_heads, group, depth).astype(jnp.float32)
    grouped_d = dout.reshape(request_block_count, length, kv_heads, group, depth).astype(jnp.float32)
    key_rows = keys.astype(jnp.float32)
    value_rows = value_matrix.astype(jnp.float32)
    scores = jnp.einsum("ntkge,nske->nkgts", grouped_q, key_rows) * (depth ** -0.5)
    scores = jnp.where(allowed[:, None, None], scores, -1e30)
    summit = jnp.max(scores, axis=-1, keepdims=True)
    expo = jnp.exp(scores - summit)
    probs = expo / jnp.sum(expo, axis=-1, keepdims=True)
    dprobs = jnp.einsum("ntkge,nske->nkgts", grouped_d, value_rows)
    dscores = probs * (dprobs - jnp.sum(dprobs * probs, axis=-1, keepdims=True))
    dscore_b = dscores.astype(jnp.bfloat16).astype(jnp.float32)
    dquery = jnp.einsum("nkgts,nske->ntkge", dscore_b, key_rows) * (depth ** -0.5)
    prob_b = probs.astype(jnp.bfloat16).astype(jnp.float32)
    dvalue = jnp.einsum("nkgts,ntkge->nske", prob_b, grouped_d)
    return dquery.reshape(request_block_count, length, heads, depth), dvalue


def reference(tokens, w_query, w_key, w_value, a_query, b_query, a_value, b_value, adapter_ranks, adapter_slot, block_adapter, live_tokens, d_heads):
    cosine, sine = rope_tables(REQUEST_ROWS, HD)
    group = HEADS // KVH
    position = jnp.arange(REQUEST_ROWS, dtype=jnp.int32)
    causal = position[None, :] <= position[:, None]
    diagonal = position[None, :] == position[:, None]
    slot_grid = jnp.arange(ADAPTERS, dtype=jnp.int32)
    rank_grid = jnp.arange(R, dtype=jnp.int32)
    row_index = jnp.arange(TOK_DEV, dtype=jnp.int32).reshape(BLOCKS_DEV, REQUEST_ROWS)

    def device_terms(carry, inputs):
        tok_rows, block_ids, count, dout_rows = inputs
        slot_ids = adapter_slot[block_ids].astype(jnp.int32)
        rank_index_list = adapter_ranks[block_ids]
        adapter_scale = (adapter_alpha_factor / rank_index_list.astype(jnp.float32))[:, None, None]
        keep = (rank_grid[None, :] < rank_index_list[:, None]).astype(jnp.float32)[:, None, :]
        block_tokens = tok_rows.reshape(BLOCKS_DEV, REQUEST_ROWS, D).astype(jnp.float32)
        aq_sel = a_query[slot_ids].astype(jnp.float32)
        av_sel = a_value[slot_ids].astype(jnp.float32)
        selected_query_up = b_query[slot_ids].astype(jnp.float32)
        selected_value_up = b_value[slot_ids].astype(jnp.float32)
        query_down_weight = (jnp.einsum("ntd,ndr->ntr", block_tokens, aq_sel) * keep).astype(jnp.bfloat16).astype(jnp.float32)
        value_down_weight = (jnp.einsum("ntd,ndr->ntr", block_tokens, av_sel) * keep).astype(jnp.bfloat16).astype(jnp.float32)
        frozen_query = jnp.dot(tok_rows, w_query, preferred_element_type=jnp.float32).reshape(BLOCKS_DEV, REQUEST_ROWS, HEADS * HD)
        full_q = frozen_query + adapter_scale * jnp.einsum("zwf,zfy->zwy", query_down_weight, selected_query_up)
        queries = rotate(full_q.reshape(BLOCKS_DEV, REQUEST_ROWS, HEADS, HD), cosine, sine).astype(jnp.bfloat16)
        base_k = jnp.dot(tok_rows, w_key, preferred_element_type=jnp.float32).reshape(BLOCKS_DEV, REQUEST_ROWS, KVH, HD)
        keys = rotate(base_k, cosine, sine).astype(jnp.bfloat16)
        frozen_value = jnp.dot(tok_rows, w_value, preferred_element_type=jnp.float32).reshape(BLOCKS_DEV, REQUEST_ROWS, KVH * HD)
        value_matrix = (frozen_value + adapter_scale * jnp.einsum("zwf,zfy->zwy", value_down_weight, selected_value_up)).astype(jnp.bfloat16)
        value_matrix = value_matrix.reshape(BLOCKS_DEV, REQUEST_ROWS, KVH, HD)
        live = row_index < count
        allowed = causal[None] & (live[:, None, :] | diagonal[None])
        dout = jnp.where(live[:, :, None], dout_rows.reshape(BLOCKS_DEV, REQUEST_ROWS, HEADS * HD), jnp.zeros((), jnp.bfloat16))
        dquery, dvalue = attention_grads(queries, keys, value_matrix, dout.reshape(BLOCKS_DEV, REQUEST_ROWS, HEADS, HD), allowed, group)
        grad_q = rotate(dquery, cosine, -sine).reshape(BLOCKS_DEV, REQUEST_ROWS, HEADS * HD).astype(jnp.bfloat16).astype(jnp.float32)
        grad_v = dvalue.reshape(BLOCKS_DEV, REQUEST_ROWS, KVH * HD).astype(jnp.bfloat16).astype(jnp.float32)
        up_q = adapter_scale * jnp.einsum("ntr,ntc->nrc", query_down_weight, grad_q)
        up_v = adapter_scale * jnp.einsum("ntr,ntc->nrc", value_down_weight, grad_v)
        back_q = (adapter_scale * jnp.einsum("ntc,nrc->ntr", grad_q, selected_query_up) * keep).astype(jnp.bfloat16).astype(jnp.float32)
        back_v = (adapter_scale * jnp.einsum("ntc,nrc->ntr", grad_v, selected_value_up) * keep).astype(jnp.bfloat16).astype(jnp.float32)
        low_q = jnp.einsum("ntd,ntr->ndr", block_tokens, back_q)
        low_v = jnp.einsum("ntd,ntr->ndr", block_tokens, back_v)
        onehot = (slot_grid[:, None] == slot_ids[None, :]).astype(jnp.float32)
        terms = (low_q, up_q, low_v, up_v)
        placed = tuple(jnp.einsum("an,nxy->axy", onehot, item).astype(jnp.bfloat16).astype(jnp.float32) for item in terms)
        return tuple(total + extra for total, extra in zip(carry, placed)), None

    start = (jnp.zeros((ADAPTERS, D, R), jnp.float32), jnp.zeros((ADAPTERS, R, HEADS * HD), jnp.float32),
             jnp.zeros((ADAPTERS, D, R), jnp.float32), jnp.zeros((ADAPTERS, R, KVH * HD), jnp.float32))
    inputs = (tokens.reshape(N_DP, TOK_DEV, D), block_adapter.reshape(N_DP, BLOCKS_DEV), live_tokens,
              d_heads.reshape(N_DP, TOK_DEV, HEADS * HD))
    totals, unused = lax.scan(device_terms, start, inputs)
    return (totals[0], totals[1], totals[2], totals[3])
```

```python
import functools

import jax
import jax.numpy as jnp
from jax import lax
from jax.experimental import pallas as pl
from jax.experimental.pallas import tpu as pltpu
from jax.sharding import PartitionSpec as P

HD = 128
R = 32
REQUEST_ROWS = 128
MESH = pl.DeviceIdType.MESH


adapter_alpha_factor = 32.0
rope_theta = 500000.0


def rope_tables(length, width):
    halfway = width // 2
    spread = rope_theta ** (-2.0 * jnp.arange(halfway, dtype=jnp.float32) / width)
    angle = jnp.arange(length, dtype=jnp.float32)[:, None] * spread[None, :]
    return (jnp.cos(angle), jnp.sin(angle))


def rotate(value_matrix, cosine, sine):
    halfway = value_matrix.shape[-1] // 2
    first = value_matrix[..., :halfway]
    second = value_matrix[..., halfway:]
    cos_grid = cosine[:, None, :]
    sin_grid = sine[:, None, :]
    return jnp.concatenate(
        [first * cos_grid - second * sin_grid, second * cos_grid + first * sin_grid], axis=-1
    )


def attention_grads(queries, keys, value_matrix, dout, allowed, group):
    request_block_count, length, heads, depth = queries.shape
    kv_heads = keys.shape[2]
    grouped_q = queries.reshape(request_block_count, length, kv_heads, group, depth)
    grouped_d = dout.reshape(request_block_count, length, kv_heads, group, depth)
    scores = jnp.einsum(
        "ntkge,nske->nkgts", grouped_q, keys, preferred_element_type=jnp.float32
    ) * depth ** (-0.5)
    scores = jnp.where(allowed[:, None, None], scores, -1e30)
    summit = jnp.max(scores, axis=-1, keepdims=True)
    expo = jnp.exp(scores - summit)
    probs = expo / jnp.sum(expo, axis=-1, keepdims=True)
    dprobs = jnp.einsum(
        "ntkge,nske->nkgts", grouped_d, value_matrix, preferred_element_type=jnp.float32
    )
    dscores = probs * (dprobs - jnp.sum(dprobs * probs, axis=-1, keepdims=True))
    dscore_b = dscores.astype(jnp.bfloat16)
    dquery = jnp.einsum(
        "nkgts,nske->ntkge", dscore_b, keys, preferred_element_type=jnp.float32
    ) * depth ** (-0.5)
    prob_b = probs.astype(jnp.bfloat16)
    dvalue = jnp.einsum("nkgts,ntkge->nske", prob_b, grouped_d, preferred_element_type=jnp.float32)
    return (dquery.reshape(request_block_count, length, heads, depth), dvalue)


def greet(axes):
    barrier = pltpu.get_barrier_semaphore()
    total = 0
    for axis in axes:
        size = lax.axis_size(axis)
        me = lax.axis_index(axis)

        @pl.loop(1, size)
        def _(j):
            pl.semaphore_signal(
                barrier, inc=1, device_id={axis: lax.rem(me + j, size)}, device_id_type=MESH
            )

        total += size - 1
    pl.semaphore_wait(barrier, total)


def project_kernel(
    pieces,
    slot_ref,
    rank_ref,
    scale_ref,
    x_hbm,
    wq_hbm,
    wk_hbm,
    wv_hbm,
    down_ref,
    bq_ref,
    bv_ref,
    acc_ref,
    u_ref,
    bq_sel_ref,
    bv_sel_ref,
    x_ref,
    w_all,
    down_all,
    bq_all,
    bv_all,
    parts,
    local_sem,
    z_send,
    z_recv,
    y_send,
    y_recv,
    f_send,
    f_recv,
    u_send,
    u_recv,
):
    n = lax.axis_size("dp")
    ng = lax.axis_size("groups")
    nt = lax.axis_size("tensor")
    me = lax.axis_index("dp")
    g = lax.axis_index("groups")
    t = lax.axis_index("tensor")
    depth = w_all.shape[1]
    cols = w_all.shape[2]
    qcols = wq_hbm.shape[1]
    kcols = wk_hbm.shape[1]
    half = depth // ng
    step = half // pieces
    rows = x_ref.shape[0]
    width = down_ref.shape[1]
    block_count = rows // REQUEST_ROWS

    x_copy = pltpu.make_async_copy(x_hbm, x_ref, local_sem.at[0])
    w_copies = [
        pltpu.make_async_copy(src, w_all.at[me, :, pl.ds(at, src.shape[1])], local_sem.at[1 + i])
        for i, (src, at) in enumerate(((wq_hbm, 0), (wk_hbm, qcols), (wv_hbm, qcols + kcols)))
    ]
    f_copies = [
        pltpu.make_async_copy(src, dst.at[me], local_sem.at[4 + i])
        for i, (src, dst) in enumerate(((down_ref, down_all), (bq_ref, bq_all), (bv_ref, bv_all)))
    ]
    for copy in w_copies + f_copies + [x_copy]:
        copy.start()
    greet(("dp", "tensor", "groups"))

    def factor_copies(j, arriving):
        peer = lax.rem(me + n - j, n) if arriving else lax.rem(me + j, n)
        at = peer if arriving else me
        return [
            pltpu.make_async_remote_copy(
                src_ref=src,
                dst_ref=dst.at[at],
                send_sem=f_send.at[i, j],
                recv_sem=f_recv.at[i, j],
                device_id={"dp": peer},
                device_id_type=MESH,
            )
            for i, (src, dst) in enumerate(
                ((down_ref, down_all), (bq_ref, bq_all), (bv_ref, bv_all))
            )
        ]

    @pl.loop(1, n)
    def _(j):
        for copy in factor_copies(j, False):
            copy.start()

    def piece(s, owner, p):
        return w_all.at[s, pl.ds(pl.multiple_of(owner * half + p * step, step), step), :]

    def z_copy(s, p, way):
        target = jnp.clip(me + (1 if way == 0 else -1), 0, n - 1)
        return pltpu.make_async_remote_copy(
            src_ref=piece(s, g, p),
            dst_ref=piece(s, g, p),
            send_sem=z_send.at[way, s, p],
            recv_sem=z_recv.at[s, p],
            device_id={"dp": target},
            device_id_type=MESH,
        )

    def y_copy(s, p, j, arriving):
        owner = lax.rem(g + ng - j, ng) if arriving else g
        return pltpu.make_async_remote_copy(
            src_ref=piece(s, owner, p),
            dst_ref=piece(s, owner, p),
            send_sem=y_send.at[j, s, p],
            recv_sem=y_recv.at[j, s, p],
            device_id={"groups": lax.rem(g + j, ng)},
            device_id_type=MESH,
        )

    for copy in w_copies:
        copy.wait()

    @pl.when(me < n - 1)
    def _():
        for p in range(pieces):
            z_copy(me, p, 0).start()

    @pl.when(me > 0)
    def _():
        for p in range(pieces):
            z_copy(me, p, 1).start()

    tile = 256 if cols % 256 == 0 else 128

    def multiply(s):
        ks = pl.ds(pl.multiple_of(s * depth, 128), depth)

        @pl.loop(0, cols // tile)
        def _(c):
            cs = pl.ds(pl.multiple_of(c * tile, tile), tile)
            acc_ref[:, cs] += jnp.dot(
                x_ref[:, ks], w_all[s, :, cs], preferred_element_type=jnp.float32
            )

    x_copy.wait()
    for copy in f_copies:
        copy.wait()
    acc_ref[...] = jnp.zeros_like(acc_ref)

    @pl.loop(1, n)
    def _(j):
        for copy in factor_copies(j, True):
            copy.wait_recv()

    mine = pl.ds(pl.multiple_of(t * width, 128), width)
    for b in range(block_count):
        span = pl.ds(b * REQUEST_ROWS, REQUEST_ROWS)
        slot = slot_ref[b]
        parts[t, span, :] = lax.dot_general(
            x_ref[span, mine],
            down_all[slot],
            (((1,), (1,)), ((), ())),
            preferred_element_type=jnp.float32,
        )
        bq_sel_ref[b] = bq_all[slot]
        bv_sel_ref[b] = bv_all[slot]

    multiply(me)

    def part_copy(j, arriving):
        peer = lax.rem(t + nt - j, nt) if arriving else lax.rem(t + j, nt)
        at = peer if arriving else t
        return pltpu.make_async_remote_copy(
            src_ref=parts.at[at],
            dst_ref=parts.at[at],
            send_sem=u_send.at[j],
            recv_sem=u_recv.at[j],
            device_id={"tensor": peer},
            device_id_type=MESH,
        )

    for j in range(1, nt):
        part_copy(j, False).start()

    def finish(s, valid):
        @pl.when(valid)
        def _():
            for p in range(pieces):
                for j in range(1, ng):
                    y_copy(s, p, j, True).wait_recv()
            multiply(s)

    def both(d):
        for p in range(pieces):
            for way in (0, 1):
                s = me - d if way == 0 else me + d
                valid = (s >= 0) if way == 0 else (s < n)
                onward = (me < n - 1) if way == 0 else (me > 0)

                @pl.when(valid)
                def _():
                    z_copy(s, p, way).wait_recv()

                    @pl.when(onward)
                    def _():
                        z_copy(s, p, way).start()

                    for j in range(1, ng):
                        y_copy(s, p, j, False).start()

    both(1)

    for j in range(1, nt):
        part_copy(j, True).wait_recv()
    for b in range(block_count):
        span = pl.ds(b * REQUEST_ROWS, REQUEST_ROWS)
        rank = rank_ref[b]
        total = parts[0, span, :]
        for j in range(1, nt):
            total = total + parts[j, span, :]
        lane = lax.broadcasted_iota(jnp.int32, total.shape, 1)
        lane = jnp.where(lane >= R, lane - R, lane)
        u = jnp.where(lane < rank, total, 0.0).astype(jnp.bfloat16)
        u_ref[span, :] = u
        acc_ref[span, :qcols] += scale_ref[b] * jnp.dot(
            u[:, :R], bq_sel_ref[b], preferred_element_type=jnp.float32
        )
        acc_ref[span, qcols + kcols :] += scale_ref[b] * jnp.dot(
            u[:, R:], bv_sel_ref[b], preferred_element_type=jnp.float32
        )

    @pl.loop(2, n + 1)
    def _(d):
        @pl.when(d < n)
        def _():
            both(d)

        finish(me - d + 1, me - d + 1 >= 0)
        finish(me + d - 1, me + d - 1 < n)

    @pl.loop(1, n)
    def _(j):
        for copy in factor_copies(j, False):
            copy.wait_send()

    for j in range(1, nt):
        part_copy(j, False).wait_send()

    @pl.loop(0, n)
    def _(s):
        for p in range(pieces):

            @pl.when((s <= me) & (me < n - 1))
            def _():
                z_copy(s, p, 0).wait_send()

            @pl.when((s >= me) & (me > 0))
            def _():
                z_copy(s, p, 1).wait_send()

            @pl.when(s != me)
            def _():
                for j in range(1, ng):
                    y_copy(s, p, j, False).wait_send()


def project(tokens, w_query, w_key, w_value, down, b_query, b_value, slots, ranks, scales):
    n, ng, nt = lax.axis_size("dp"), lax.axis_size("groups"), lax.axis_size("tensor")
    rows = tokens.shape[0]
    depth, qcols = w_query.shape
    kcols = w_key.shape[1]
    cols = qcols + 2 * kcols
    half = depth // ng
    pieces = max(1, half // 128)
    blocks = rows // REQUEST_ROWS
    smem = pl.BlockSpec(memory_space=pltpu.SMEM)
    vmem = pl.BlockSpec(memory_space=pltpu.VMEM)
    hbm = pl.BlockSpec(memory_space=pltpu.HBM)
    dma = pltpu.SemaphoreType.DMA
    return pl.pallas_call(
        functools.partial(project_kernel, pieces),
        out_shape=(
            jax.ShapeDtypeStruct((rows, cols), jnp.float32),
            jax.ShapeDtypeStruct((rows, 2 * R), jnp.bfloat16),
            jax.ShapeDtypeStruct((blocks, R, qcols), jnp.bfloat16),
            jax.ShapeDtypeStruct((blocks, R, kcols), jnp.bfloat16),
        ),
        in_specs=[smem] * 3 + [hbm] * 4 + [vmem] * 3,
        out_specs=(vmem,) * 4,
        scratch_shapes=[
            pltpu.VMEM(tokens.shape, jnp.bfloat16),
            pltpu.VMEM((n, depth, cols), jnp.bfloat16),
            pltpu.VMEM((n,) + down.shape, jnp.bfloat16),
            pltpu.VMEM((n,) + b_query.shape, jnp.bfloat16),
            pltpu.VMEM((n,) + b_value.shape, jnp.bfloat16),
            pltpu.VMEM((nt, rows, 2 * R), jnp.float32),
            dma((7,)),
            dma((2, n, pieces)),
            dma((n, pieces)),
            dma((ng, n, pieces)),
            dma((ng, n, pieces)),
            dma((3, n)),
            dma((3, n)),
            dma((nt,)),
            dma((nt,)),
        ],
        compiler_params=pltpu.CompilerParams(
            collective_id=0, has_side_effects=True, vmem_limit_bytes=60 * 1024 * 1024
        ),
        name="project",
    )(slots, ranks, scales, tokens, w_query, w_key, w_value, down, b_query, b_value)


def reduce_kernel(
    x_ref,
    mask_ref,
    keep_ref,
    part_ref,
    upq_ref,
    upv_ref,
    low_out,
    upq_out,
    upv_out,
    backs,
    low_send,
    low_got,
    upq_got,
    upv_got,
    b_send,
    b_recv,
    a_send,
    a_recv,
):
    n, nt = lax.axis_size("dp"), lax.axis_size("tensor")
    me, t = lax.axis_index("dp"), lax.axis_index("tensor")
    greet(("dp", "tensor"))

    def back_copy(j, arriving):
        peer = lax.rem(t + nt - j, nt) if arriving else lax.rem(t + j, nt)
        at = peer if arriving else t
        return pltpu.make_async_remote_copy(
            src_ref=part_ref,
            dst_ref=backs.at[at],
            send_sem=b_send.at[j],
            recv_sem=b_recv.at[j],
            device_id={"tensor": peer},
            device_id_type=MESH,
        )

    def grad_copy(i, src, dst, j, arriving):
        peer = lax.rem(me + n - j, n) if arriving else lax.rem(me + j, n)
        at = peer if arriving else me
        return pltpu.make_async_remote_copy(
            src_ref=src.at[peer],
            dst_ref=dst.at[at],
            send_sem=a_send.at[i, j],
            recv_sem=a_recv.at[i, j],
            device_id={"dp": peer},
            device_id_type=MESH,
        )

    trio = ((0, upq_ref, upq_got), (1, upv_ref, upv_got), (2, low_send, low_got))
    for j in range(1, nt):
        back_copy(j, False).start()

    @pl.loop(1, n)
    def _(j):
        for i, src, dst in trio[:2]:
            grad_copy(i, src, dst, j, False).start()

    backs[t] = part_ref[...]
    for j in range(1, nt):
        back_copy(j, True).wait_recv()
    total = backs[0].astype(jnp.float32)
    for j in range(1, nt):
        total = total + backs[j].astype(jnp.float32)
    back = (total * keep_ref[...]).astype(jnp.bfloat16)

    @pl.loop(1, n + 1)
    def _(j):
        a = lax.rem(me + j, n)
        chosen = (mask_ref[a] * back).astype(jnp.bfloat16)
        low_send[a] = lax.dot_general(
            chosen, x_ref[...], (((0,), (0,)), ((), ())), preferred_element_type=jnp.float32
        ).astype(jnp.bfloat16)

        @pl.when(j < n)
        def _():
            grad_copy(2, low_send, low_got, j, False).start()

    low_got[me] = low_send[me]
    upq_got[me] = upq_ref[me]
    upv_got[me] = upv_ref[me]

    for i, src, dst in trio:

        @pl.loop(1, n)
        def _(j):
            grad_copy(i, src, dst, j, True).wait_recv()

    for got, out in ((low_got, low_out), (upq_got, upq_out), (upv_got, upv_out)):
        out[...] = jnp.zeros_like(out)

        @pl.loop(0, n)
        def _(s):
            out[...] += got[s].astype(jnp.float32)

    for j in range(1, nt):
        back_copy(j, False).wait_send()

    for i, src, dst in trio:

        @pl.loop(1, n)
        def _(j):
            grad_copy(i, src, dst, j, False).wait_send()


def reduce_grads(x_local, mask, keep, part, up_q, up_v):
    n, nt = lax.axis_size("dp"), lax.axis_size("tensor")
    rows, width = x_local.shape
    vmem = pl.BlockSpec(memory_space=pltpu.VMEM)
    dma = pltpu.SemaphoreType.DMA
    low_shape = (n, 2 * R, width)
    return pl.pallas_call(
        reduce_kernel,
        out_shape=(
            jax.ShapeDtypeStruct(low_shape[1:], jnp.float32),
            jax.ShapeDtypeStruct(up_q.shape[1:], jnp.float32),
            jax.ShapeDtypeStruct(up_v.shape[1:], jnp.float32),
        ),
        in_specs=[vmem] * 6,
        out_specs=(vmem,) * 3,
        scratch_shapes=[
            pltpu.VMEM((nt,) + part.shape, jnp.bfloat16),
            pltpu.VMEM(low_shape, jnp.bfloat16),
            pltpu.VMEM(low_shape, jnp.bfloat16),
            pltpu.VMEM(up_q.shape, jnp.bfloat16),
            pltpu.VMEM(up_v.shape, jnp.bfloat16),
            dma((nt,)),
            dma((nt,)),
            dma((3, n)),
            dma((3, n)),
        ],
        compiler_params=pltpu.CompilerParams(
            collective_id=1, has_side_effects=True, vmem_limit_bytes=60 * 1024 * 1024
        ),
        name="reduce_grads",
    )(x_local, mask, keep, part, up_q, up_v)


def on_device(
    tokens,
    w_query,
    w_key,
    w_value,
    a_query,
    b_query,
    a_value,
    b_value,
    adapter_ranks,
    adapter_slot,
    block_adapter,
    live_tokens,
    d_heads,
):
    row_count = tokens.shape[0]
    request_block_count = row_count // REQUEST_ROWS
    local_width = a_query.shape[1]
    query_column_count = w_query.shape[1]
    value_column_count = w_key.shape[1]
    local_heads = query_column_count // HD
    local_kv = value_column_count // HD
    group = local_heads // local_kv
    dp_count = lax.axis_size("dp")
    owned = a_query.shape[0]
    adapter_count = owned * dp_count
    cosine, sine = rope_tables(REQUEST_ROWS, HD)
    column_start = lax.axis_index("tensor") * local_width
    tok_local = lax.dynamic_slice_in_dim(tokens, column_start, local_width, 1)
    block_ids = block_adapter[:, 0]
    slot_ids = adapter_slot[block_ids]
    rank_index_list = adapter_ranks[block_ids]
    scales = adapter_alpha_factor / rank_index_list.astype(jnp.float32)
    adapter_scale = scales[:, None, None]
    keep = (jnp.arange(R, dtype=jnp.int32)[None, :] < rank_index_list[:, None]).astype(jnp.float32)
    down = jnp.concatenate([a_query[0].T, a_value[0].T], axis=0)
    full, low_rank, selected_query_up, selected_value_up = project(
        tokens, w_query, w_key, w_value, down, b_query[0], b_value[0],
        slot_ids, rank_index_list, scales,
    )
    shape3 = (request_block_count, REQUEST_ROWS, -1)
    query_down_weight = low_rank[:, :R].reshape(shape3)
    value_down_weight = low_rank[:, R:].reshape(shape3)
    queries = rotate(
        full[:, :query_column_count].reshape(request_block_count, REQUEST_ROWS, local_heads, HD),
        cosine, sine,
    ).astype(jnp.bfloat16)
    keys = rotate(
        full[:, query_column_count : query_column_count + value_column_count].reshape(
            request_block_count, REQUEST_ROWS, local_kv, HD
        ),
        cosine, sine,
    ).astype(jnp.bfloat16)
    value_matrix = full[:, query_column_count + value_column_count :].astype(jnp.bfloat16)
    value_matrix = value_matrix.reshape(request_block_count, REQUEST_ROWS, local_kv, HD)
    position = jnp.arange(REQUEST_ROWS, dtype=jnp.int32)
    causal = position[None, :] <= position[:, None]
    diagonal = position[None, :] == position[:, None]
    row_index = jnp.arange(row_count, dtype=jnp.int32).reshape(request_block_count, REQUEST_ROWS)
    live = row_index < live_tokens[0]
    allowed = causal[None] & (live[:, None, :] | diagonal[None])
    dout = jnp.where(
        live[:, :, None],
        d_heads.reshape(request_block_count, REQUEST_ROWS, query_column_count),
        jnp.zeros((), jnp.bfloat16),
    )
    dquery, dvalue = attention_grads(
        queries,
        keys,
        value_matrix,
        dout.reshape(request_block_count, REQUEST_ROWS, local_heads, HD),
        allowed,
        group,
    )
    grad_q = (
        rotate(dquery, cosine, -sine)
        .reshape(request_block_count, REQUEST_ROWS, query_column_count)
        .astype(jnp.bfloat16)
    )
    grad_v = dvalue.reshape(request_block_count, REQUEST_ROWS, value_column_count).astype(
        jnp.bfloat16
    )
    up_q = adapter_scale * jnp.einsum(
        "ntr,ntc->nrc", query_down_weight, grad_q, preferred_element_type=jnp.float32
    )
    up_v = adapter_scale * jnp.einsum(
        "ntr,ntc->nrc", value_down_weight, grad_v, preferred_element_type=jnp.float32
    )
    part_back_q = adapter_scale * jnp.einsum(
        "ntc,nrc->ntr", grad_q, selected_query_up, preferred_element_type=jnp.float32
    )
    part_back_v = adapter_scale * jnp.einsum(
        "ntc,nrc->ntr", grad_v, selected_value_up, preferred_element_type=jnp.float32
    )
    part_back = jnp.concatenate([part_back_q, part_back_v], axis=-1)
    part_back = part_back.reshape(row_count, 2 * R).astype(jnp.bfloat16)
    chosen = jnp.arange(adapter_count, dtype=jnp.int32)[:, None] == slot_ids[None, :]
    onehot = chosen.astype(jnp.float32)
    placed_q, placed_v = (
        jnp.einsum("an,nxy->axy", onehot, item).astype(jnp.bfloat16) for item in (up_q, up_v)
    )
    row_mask = jnp.broadcast_to(
        chosen[:, :, None, None], (adapter_count, request_block_count, REQUEST_ROWS, 2 * R)
    ).reshape(adapter_count, row_count, 2 * R).astype(jnp.bfloat16)
    row_keep = jnp.broadcast_to(
        jnp.concatenate([keep, keep], axis=-1)[:, None, :],
        (request_block_count, REQUEST_ROWS, 2 * R),
    ).reshape(row_count, 2 * R)
    low, grad_bq, grad_bv = reduce_grads(
        tok_local, row_mask, row_keep, part_back, placed_q, placed_v
    )
    return (low[:R].T[None], grad_bq[None], low[R:].T[None], grad_bv[None])


def solution(mesh):
    in_specs = (
        P(("groups", "dp"), None),
        P("dp", "tensor"),
        P("dp", "tensor"),
        P("dp", "tensor"),
        P(("groups", "dp"), "tensor", None),
        P(("groups", "dp"), None, "tensor"),
        P(("groups", "dp"), "tensor", None),
        P(("groups", "dp"), None, "tensor"),
        P("groups"),
        P(),
        P(("groups", "dp"), None),
        P(("groups", "dp")),
        P(("groups", "dp"), "tensor"),
    )
    out_specs = (
        P(("groups", "dp"), "tensor", None),
        P(("groups", "dp"), None, "tensor"),
        P(("groups", "dp"), "tensor", None),
        P(("groups", "dp"), None, "tensor"),
    )
    return jax.shard_map(
        on_device, mesh=mesh, in_specs=in_specs, out_specs=out_specs, check_vma=False
    )
```

```python
import functools

import jax
import jax.numpy as jnp
import numpy as np
from jax import lax
from jax.experimental import pallas as pl
from jax.experimental.pallas import tpu as pltpu
from jax.sharding import PartitionSpec as P

HD = 128
R = 32
REQUEST_ROWS = 128
MESH = pl.DeviceIdType.MESH


adapter_alpha_factor = 32.0
rope_theta = 500000.0


def rope_tables(length, width):
    halfway = width // 2
    spread = rope_theta ** (-2.0 * np.arange(halfway, dtype=np.float32) / width)
    angle = np.arange(length, dtype=np.float32)[:, None] * spread.astype(np.float32)[None, :]
    return np.cos(angle).astype(np.float32), np.sin(angle).astype(np.float32)


def scale_of(rank):
    return (adapter_alpha_factor / jnp.full((1, 128), rank, jnp.int32).astype(jnp.float32))[:, :1]


def greet(axes):
    barrier = pltpu.get_barrier_semaphore()
    total = 0
    for axis in axes:
        size = lax.axis_size(axis)
        me = lax.axis_index(axis)

        @pl.loop(1, size)
        def _(j):
            pl.semaphore_signal(
                barrier, inc=1, device_id={axis: lax.rem(me + j, size)}, device_id_type=MESH
            )

        total += size - 1
    pl.semaphore_wait(barrier, total)


def project_kernel(
    pieces,
    block_ref,
    slot_ref,
    rank_ref,
    x_hbm,
    wq_hbm,
    wk_hbm,
    wv_hbm,
    down_ref,
    bq_ref,
    bv_ref,
    acc_ref,
    u_ref,
    bq_sel_ref,
    bv_sel_ref,
    x_ref,
    w_all,
    down_all,
    bq_all,
    bv_all,
    parts,
    local_sem,
    z_send,
    z_recv,
    y_send,
    y_recv,
    f_send,
    f_recv,
    u_send,
    u_recv,
):
    n = lax.axis_size("dp")
    ng = lax.axis_size("groups")
    nt = lax.axis_size("tensor")
    me = lax.axis_index("dp")
    g = lax.axis_index("groups")
    t = lax.axis_index("tensor")
    depth = w_all.shape[1]
    cols = w_all.shape[2]
    qcols = wq_hbm.shape[1]
    kcols = wk_hbm.shape[1]
    half = depth // ng
    step = half // pieces
    rows = x_ref.shape[0]
    width = down_ref.shape[1]
    block_count = rows // REQUEST_ROWS

    x_copy = pltpu.make_async_copy(x_hbm, x_ref, local_sem.at[0])
    w_copies = [
        pltpu.make_async_copy(src, w_all.at[me, :, pl.ds(at, src.shape[1])], local_sem.at[1 + i])
        for i, (src, at) in enumerate(((wq_hbm, 0), (wk_hbm, qcols), (wv_hbm, qcols + kcols)))
    ]
    f_copies = [
        pltpu.make_async_copy(src, dst.at[me], local_sem.at[4 + i])
        for i, (src, dst) in enumerate(((down_ref, down_all), (bq_ref, bq_all), (bv_ref, bv_all)))
    ]
    for copy in w_copies + f_copies + [x_copy]:
        copy.start()
    greet(("dp", "tensor", "groups"))

    def factor_copies(j, arriving):
        peer = lax.rem(me + n - j, n) if arriving else lax.rem(me + j, n)
        at = peer if arriving else me
        return [
            pltpu.make_async_remote_copy(
                src_ref=src,
                dst_ref=dst.at[at],
                send_sem=f_send.at[i, j],
                recv_sem=f_recv.at[i, j],
                device_id={"dp": peer},
                device_id_type=MESH,
            )
            for i, (src, dst) in enumerate(
                ((down_ref, down_all), (bq_ref, bq_all), (bv_ref, bv_all))
            )
        ]

    @pl.loop(1, n)
    def _(j):
        for copy in factor_copies(j, False):
            copy.start()

    def piece(s, owner, p):
        return w_all.at[s, pl.ds(pl.multiple_of(owner * half + p * step, step), step), :]

    def z_copy(s, p, way):
        target = jnp.clip(me + (1 if way == 0 else -1), 0, n - 1)
        return pltpu.make_async_remote_copy(
            src_ref=piece(s, g, p),
            dst_ref=piece(s, g, p),
            send_sem=z_send.at[way, s, p],
            recv_sem=z_recv.at[s, p],
            device_id={"dp": target},
            device_id_type=MESH,
        )

    def y_copy(s, p, j, arriving):
        owner = lax.rem(g + ng - j, ng) if arriving else g
        return pltpu.make_async_remote_copy(
            src_ref=piece(s, owner, p),
            dst_ref=piece(s, owner, p),
            send_sem=y_send.at[j, s, p],
            recv_sem=y_recv.at[j, s, p],
            device_id={"groups": lax.rem(g + j, ng)},
            device_id_type=MESH,
        )

    for copy in w_copies:
        copy.wait()

    @pl.when(me < n - 1)
    def _():
        for p in range(pieces):
            z_copy(me, p, 0).start()

    @pl.when(me > 0)
    def _():
        for p in range(pieces):
            z_copy(me, p, 1).start()

    tile = 256 if cols % 256 == 0 else 128

    def multiply(s):
        ks = pl.ds(pl.multiple_of(s * depth, 128), depth)

        @pl.loop(0, cols // tile)
        def _(c):
            cs = pl.ds(pl.multiple_of(c * tile, tile), tile)
            acc_ref[:, cs] += jnp.dot(
                x_ref[:, ks], w_all[s, :, cs], preferred_element_type=jnp.float32
            )

    x_copy.wait()
    for copy in f_copies:
        copy.wait()
    acc_ref[...] = jnp.zeros_like(acc_ref)

    @pl.loop(1, n)
    def _(j):
        for copy in factor_copies(j, True):
            copy.wait_recv()

    mine = pl.ds(pl.multiple_of(t * width, 128), width)
    for b in range(block_count):
        span = pl.ds(b * REQUEST_ROWS, REQUEST_ROWS)
        slot = slot_ref[block_ref[b, 0]]
        parts[t, span, :] = lax.dot_general(
            x_ref[span, mine],
            down_all[slot],
            (((1,), (1,)), ((), ())),
            preferred_element_type=jnp.float32,
        )
        bq_sel_ref[b] = bq_all[slot]
        bv_sel_ref[b] = bv_all[slot]

    multiply(me)

    def part_copy(j, arriving):
        peer = lax.rem(t + nt - j, nt) if arriving else lax.rem(t + j, nt)
        at = peer if arriving else t
        return pltpu.make_async_remote_copy(
            src_ref=parts.at[at],
            dst_ref=parts.at[at],
            send_sem=u_send.at[j],
            recv_sem=u_recv.at[j],
            device_id={"tensor": peer},
            device_id_type=MESH,
        )

    for j in range(1, nt):
        part_copy(j, False).start()

    def finish(s, valid):
        @pl.when(valid)
        def _():
            for p in range(pieces):
                for j in range(1, ng):
                    y_copy(s, p, j, True).wait_recv()
            multiply(s)

    def both(d):
        for p in range(pieces):
            for way in (0, 1):
                s = me - d if way == 0 else me + d
                valid = (s >= 0) if way == 0 else (s < n)
                onward = (me < n - 1) if way == 0 else (me > 0)

                @pl.when(valid)
                def _():
                    z_copy(s, p, way).wait_recv()

                    @pl.when(onward)
                    def _():
                        z_copy(s, p, way).start()

                    for j in range(1, ng):
                        y_copy(s, p, j, False).start()

    both(1)

    for j in range(1, nt):
        part_copy(j, True).wait_recv()
    for b in range(block_count):
        span = pl.ds(b * REQUEST_ROWS, REQUEST_ROWS)
        rank = rank_ref[block_ref[b, 0]]
        scale = scale_of(rank)
        total = parts[0, span, :]
        for j in range(1, nt):
            total = total + parts[j, span, :]
        lane = lax.broadcasted_iota(jnp.int32, total.shape, 1)
        lane = jnp.where(lane >= R, lane - R, lane)
        u = jnp.where(lane < rank, total, 0.0).astype(jnp.bfloat16)
        u_ref[span, :] = u
        acc_ref[span, :qcols] += scale * jnp.dot(
            u[:, :R], bq_sel_ref[b], preferred_element_type=jnp.float32
        )
        acc_ref[span, qcols + kcols :] += scale * jnp.dot(
            u[:, R:], bv_sel_ref[b], preferred_element_type=jnp.float32
        )

    @pl.loop(2, n + 1)
    def _(d):
        @pl.when(d < n)
        def _():
            both(d)

        finish(me - d + 1, me - d + 1 >= 0)
        finish(me + d - 1, me + d - 1 < n)

    @pl.loop(1, n)
    def _(j):
        for copy in factor_copies(j, False):
            copy.wait_send()

    for j in range(1, nt):
        part_copy(j, False).wait_send()

    @pl.loop(0, n)
    def _(s):
        for p in range(pieces):

            @pl.when((s <= me) & (me < n - 1))
            def _():
                z_copy(s, p, 0).wait_send()

            @pl.when((s >= me) & (me > 0))
            def _():
                z_copy(s, p, 1).wait_send()

            @pl.when(s != me)
            def _():
                for j in range(1, ng):
                    y_copy(s, p, j, False).wait_send()


def project(tokens, w_query, w_key, w_value, down, b_query, b_value, blocks_of, slots, ranks):
    n, ng, nt = lax.axis_size("dp"), lax.axis_size("groups"), lax.axis_size("tensor")
    rows = tokens.shape[0]
    depth, qcols = w_query.shape
    kcols = w_key.shape[1]
    cols = qcols + 2 * kcols
    half = depth // ng
    pieces = max(1, half // 128)
    blocks = rows // REQUEST_ROWS
    smem = pl.BlockSpec(memory_space=pltpu.SMEM)
    vmem = pl.BlockSpec(memory_space=pltpu.VMEM)
    hbm = pl.BlockSpec(memory_space=pltpu.HBM)
    dma = pltpu.SemaphoreType.DMA
    return pl.pallas_call(
        functools.partial(project_kernel, pieces),
        out_shape=(
            jax.ShapeDtypeStruct((rows, cols), jnp.float32),
            jax.ShapeDtypeStruct((rows, 2 * R), jnp.bfloat16),
            jax.ShapeDtypeStruct((blocks, R, qcols), jnp.bfloat16),
            jax.ShapeDtypeStruct((blocks, R, kcols), jnp.bfloat16),
        ),
        in_specs=[smem] * 3 + [hbm] * 4 + [vmem] * 3,
        out_specs=(vmem,) * 4,
        scratch_shapes=[
            pltpu.VMEM(tokens.shape, jnp.bfloat16),
            pltpu.VMEM((n, depth, cols), jnp.bfloat16),
            pltpu.VMEM((n,) + down.shape, jnp.bfloat16),
            pltpu.VMEM((n,) + b_query.shape, jnp.bfloat16),
            pltpu.VMEM((n,) + b_value.shape, jnp.bfloat16),
            pltpu.VMEM((nt, rows, 2 * R), jnp.float32),
            dma((7,)),
            dma((2, n, pieces)),
            dma((n, pieces)),
            dma((ng, n, pieces)),
            dma((ng, n, pieces)),
            dma((3, n)),
            dma((3, n)),
            dma((nt,)),
            dma((nt,)),
        ],
        compiler_params=pltpu.CompilerParams(
            collective_id=0, has_side_effects=True, vmem_limit_bytes=60 * 1024 * 1024
        ),
        name="project",
    )(blocks_of, slots, ranks, tokens, w_query, w_key, w_value, down, b_query, b_value)


def reduce_kernel(
    block_ref,
    slot_ref,
    rank_ref,
    x_hbm,
    part_ref,
    upq_ref,
    upv_ref,
    low_out,
    upq_out,
    upv_out,
    x_ref,
    back_ref,
    x_sem,
    backs,
    low_send,
    low_got,
    upq_got,
    upv_got,
    b_send,
    b_recv,
    a_send,
    a_recv,
):
    n, nt = lax.axis_size("dp"), lax.axis_size("tensor")
    me, t = lax.axis_index("dp"), lax.axis_index("tensor")
    width = x_ref.shape[1]
    block_count = x_ref.shape[0] // REQUEST_ROWS
    x_copy = pltpu.make_async_copy(
        x_hbm.at[:, pl.ds(pl.multiple_of(t * width, 128), width)], x_ref, x_sem
    )
    x_copy.start()
    greet(("dp", "tensor"))

    def back_copy(j, arriving):
        peer = lax.rem(t + nt - j, nt) if arriving else lax.rem(t + j, nt)
        at = peer if arriving else t
        return pltpu.make_async_remote_copy(
            src_ref=part_ref,
            dst_ref=backs.at[at],
            send_sem=b_send.at[j],
            recv_sem=b_recv.at[j],
            device_id={"tensor": peer},
            device_id_type=MESH,
        )

    def grad_copy(i, src, dst, j, arriving):
        peer = lax.rem(me + n - j, n) if arriving else lax.rem(me + j, n)
        at = peer if arriving else me
        return pltpu.make_async_remote_copy(
            src_ref=src.at[peer],
            dst_ref=dst.at[at],
            send_sem=a_send.at[i, j],
            recv_sem=a_recv.at[i, j],
            device_id={"dp": peer},
            device_id_type=MESH,
        )

    trio = ((0, upq_ref, upq_got), (1, upv_ref, upv_got), (2, low_send, low_got))
    for j in range(1, nt):
        back_copy(j, False).start()

    @pl.loop(1, n)
    def _(j):
        for i, src, dst in trio[:2]:
            grad_copy(i, src, dst, j, False).start()

    backs[t] = part_ref[...]
    for j in range(1, nt):
        back_copy(j, True).wait_recv()
    total = backs[0].astype(jnp.float32)
    for j in range(1, nt):
        total = total + backs[j].astype(jnp.float32)
    lane = lax.broadcasted_iota(jnp.int32, (REQUEST_ROWS, 2 * R), 1)
    lane = jnp.where(lane >= R, lane - R, lane)
    for b in range(block_count):
        span = pl.ds(b * REQUEST_ROWS, REQUEST_ROWS)
        kept = total[b * REQUEST_ROWS : (b + 1) * REQUEST_ROWS]
        back_ref[span, :] = jnp.where(lane < rank_ref[block_ref[b, 0]], kept, 0.0)
    x_copy.wait()

    @pl.loop(1, n + 1)
    def _(j):
        a = lax.rem(me + j, n)
        chosen = jnp.concatenate(
            [
                jnp.where(
                    jnp.full((REQUEST_ROWS, 2 * R), slot_ref[block_ref[b, 0]], jnp.int32) == a,
                    back_ref[pl.ds(b * REQUEST_ROWS, REQUEST_ROWS), :],
                    0.0,
                )
                for b in range(block_count)
            ],
            axis=0,
        ).astype(jnp.bfloat16)
        low_send[a] = lax.dot_general(
            chosen, x_ref[...], (((0,), (0,)), ((), ())), preferred_element_type=jnp.float32
        ).astype(jnp.bfloat16)

        @pl.when(j < n)
        def _():
            grad_copy(2, low_send, low_got, j, False).start()

    low_got[me] = low_send[me]
    upq_got[me] = upq_ref[me]
    upv_got[me] = upv_ref[me]

    for i, src, dst in trio:

        @pl.loop(1, n)
        def _(j):
            grad_copy(i, src, dst, j, True).wait_recv()

    for got, out in ((low_got, low_out), (upq_got, upq_out), (upv_got, upv_out)):
        out[...] = jnp.zeros_like(out)

        @pl.loop(0, n)
        def _(s):
            out[...] += got[s].astype(jnp.float32)

    for j in range(1, nt):
        back_copy(j, False).wait_send()

    for i, src, dst in trio:

        @pl.loop(1, n)
        def _(j):
            grad_copy(i, src, dst, j, False).wait_send()


def reduce_grads(tokens, width, blocks_of, slots, ranks, part, up_q, up_v):
    n, nt = lax.axis_size("dp"), lax.axis_size("tensor")
    rows = tokens.shape[0]
    smem = pl.BlockSpec(memory_space=pltpu.SMEM)
    hbm = pl.BlockSpec(memory_space=pltpu.HBM)
    vmem = pl.BlockSpec(memory_space=pltpu.VMEM)
    dma = pltpu.SemaphoreType.DMA
    low_shape = (n, 2 * R, width)
    return pl.pallas_call(
        reduce_kernel,
        out_shape=(
            jax.ShapeDtypeStruct(low_shape[1:], jnp.float32),
            jax.ShapeDtypeStruct(up_q.shape[1:], jnp.float32),
            jax.ShapeDtypeStruct(up_v.shape[1:], jnp.float32),
        ),
        in_specs=[smem] * 3 + [hbm] + [vmem] * 3,
        out_specs=(vmem,) * 3,
        scratch_shapes=[
            pltpu.VMEM((rows, width), jnp.bfloat16),
            pltpu.VMEM((rows, 2 * R), jnp.float32),
            dma,
            pltpu.VMEM((nt,) + part.shape, jnp.bfloat16),
            pltpu.VMEM(low_shape, jnp.bfloat16),
            pltpu.VMEM(low_shape, jnp.bfloat16),
            pltpu.VMEM(up_q.shape, jnp.bfloat16),
            pltpu.VMEM(up_v.shape, jnp.bfloat16),
            dma((nt,)),
            dma((nt,)),
            dma((3, n)),
            dma((3, n)),
        ],
        compiler_params=pltpu.CompilerParams(
            collective_id=1, has_side_effects=True, vmem_limit_bytes=60 * 1024 * 1024
        ),
        name="reduce_grads",
    )(blocks_of, slots, ranks, tokens, part, up_q, up_v)

def attend_kernel(
    group,
    block_ref,
    slot_ref,
    rank_ref,
    live_ref,
    cos_ref,
    sin_ref,
    q_ref,
    kv_ref,
    u_ref,
    bq_ref,
    bv_ref,
    d_ref,
    part_ref,
    upq_ref,
    upv_ref,
    gq_ref,
    gv_ref,
    upq_sum,
    upv_sum,
):
    b = pl.program_id(0)
    kcols = kv_ref.shape[1] // 2
    kv_heads = kcols // HD
    adapter = block_ref[b, 0]
    slot = slot_ref[adapter]
    scale = scale_of(rank_ref[adapter])
    live = live_ref[0] - b * REQUEST_ROWS

    @pl.when(b == 0)
    def _():
        upq_sum[...] = jnp.zeros_like(upq_sum)
        upv_sum[...] = jnp.zeros_like(upv_sum)

    cosine, sine = cos_ref[...], sin_ref[...]
    dims = (REQUEST_ROWS, REQUEST_ROWS)
    query_at = lax.broadcasted_iota(jnp.int32, dims, 0)
    key_at = lax.broadcasted_iota(jnp.int32, dims, 1)
    allowed = (key_at <= query_at) & ((key_at < live) | (key_at == query_at))
    allowed = jnp.concatenate([allowed.astype(jnp.float32)] * group, axis=0) > 0.5
    live_rows = lax.broadcasted_iota(jnp.int32, (REQUEST_ROWS, HD), 0) < live

    def turn(item, sign):
        return item * cosine + pltpu.roll(item, HD // 2, 1) * (sign * sine)

    def dot(a, c, left, right):
        return lax.dot_general(
            a, c, (((left,), (right,)), ((), ())), preferred_element_type=jnp.float32
        )

    for k in range(kv_heads):
        keys = turn(kv_ref[:, k * HD : (k + 1) * HD], 1.0).astype(jnp.bfloat16)
        values = kv_ref[:, kcols + k * HD : kcols + (k + 1) * HD].astype(jnp.bfloat16)
        heads = [pl.ds((k * group + i) * HD, HD) for i in range(group)]
        queries = jnp.concatenate(
            [turn(q_ref[:, h], 1.0).astype(jnp.bfloat16) for h in heads], axis=0
        )
        dout = jnp.concatenate(
            [
                jnp.where(live_rows, d_ref[:, h].astype(jnp.float32), 0.0).astype(jnp.bfloat16)
                for h in heads
            ],
            axis=0,
        )
        scores = dot(queries, keys, 1, 1) * HD ** (-0.5)
        scores = jnp.where(allowed, scores, -1e30)
        expo = jnp.exp(scores - jnp.max(scores, axis=-1, keepdims=True))
        probs = expo / jnp.sum(expo, axis=-1, keepdims=True)
        dprobs = dot(dout, values, 1, 1)
        dscores = probs * (dprobs - jnp.sum(dprobs * probs, axis=-1, keepdims=True))
        dquery = dot(dscores.astype(jnp.bfloat16), keys, 1, 0) * HD ** (-0.5)
        for i, h in enumerate(heads):
            rows = dquery[i * REQUEST_ROWS : (i + 1) * REQUEST_ROWS]
            gq_ref[:, h] = turn(rows, -1.0).astype(jnp.bfloat16)
        gv_ref[:, k * HD : (k + 1) * HD] = dot(probs.astype(jnp.bfloat16), dout, 0, 0).astype(
            jnp.bfloat16
        )
    u = u_ref[...]
    upq_sum[slot] += scale * dot(u[:, :R], gq_ref[...], 0, 0)
    upv_sum[slot] += scale * dot(u[:, R:], gv_ref[...], 0, 0)
    part_ref[...] = (
        scale
        * jnp.concatenate(
            [dot(gq_ref[...], bq_ref[0], 1, 1), dot(gv_ref[...], bv_ref[0], 1, 1)], axis=-1
        )
    ).astype(jnp.bfloat16)

    @pl.when(b == pl.num_programs(0) - 1)
    def _():
        upq_ref[...] = upq_sum[...].astype(jnp.bfloat16)
        upv_ref[...] = upv_sum[...].astype(jnp.bfloat16)


def attend(full, low_rank, up_query, up_value, d_heads, blocks_of, slots, ranks, live):
    slot_count = slots.shape[0]
    rows, qcols = d_heads.shape
    kcols = up_value.shape[2]
    group = qcols // kcols
    cosine, sine = rope_tables(REQUEST_ROWS, HD)
    cosine = np.concatenate([cosine, cosine], axis=-1)
    sine = np.concatenate([-sine, sine], axis=-1)
    smem = pl.BlockSpec(memory_space=pltpu.SMEM)
    table = pl.BlockSpec((REQUEST_ROWS, HD), lambda b: (0, 0))
    upq_shape = (slot_count, R, qcols)
    upv_shape = (slot_count, R, kcols)
    ratio = qcols // (2 * kcols)
    return pl.pallas_call(
        functools.partial(attend_kernel, group),
        grid=(rows // REQUEST_ROWS,),
        out_shape=(
            jax.ShapeDtypeStruct((rows, 2 * R), jnp.bfloat16),
            jax.ShapeDtypeStruct(upq_shape, jnp.bfloat16),
            jax.ShapeDtypeStruct(upv_shape, jnp.bfloat16),
        ),
        in_specs=[smem] * 4
        + [
            table,
            table,
            pl.BlockSpec((REQUEST_ROWS, qcols), lambda b: (b, 0)),
            pl.BlockSpec((REQUEST_ROWS, 2 * kcols), lambda b: (b, ratio)),
            pl.BlockSpec((REQUEST_ROWS, 2 * R), lambda b: (b, 0)),
            pl.BlockSpec((1, R, qcols), lambda b: (b, 0, 0)),
            pl.BlockSpec((1, R, kcols), lambda b: (b, 0, 0)),
            pl.BlockSpec((REQUEST_ROWS, qcols), lambda b: (b, 0)),
        ],
        out_specs=(
            pl.BlockSpec((REQUEST_ROWS, 2 * R), lambda b: (b, 0)),
            pl.BlockSpec(upq_shape, lambda b: (0, 0, 0)),
            pl.BlockSpec(upv_shape, lambda b: (0, 0, 0)),
        ),
        scratch_shapes=[
            pltpu.VMEM((REQUEST_ROWS, qcols), jnp.bfloat16),
            pltpu.VMEM((REQUEST_ROWS, kcols), jnp.bfloat16),
            pltpu.VMEM(upq_shape, jnp.float32),
            pltpu.VMEM(upv_shape, jnp.float32),
        ],
        name="attend",
    )(
        blocks_of, slots, ranks, live, cosine, sine, full, full, low_rank, up_query, up_value, d_heads
    )


def on_device(
    tokens,
    w_query,
    w_key,
    w_value,
    a_query,
    b_query,
    a_value,
    b_value,
    adapter_ranks,
    adapter_slot,
    block_adapter,
    live_tokens,
    d_heads,
):
    width = a_query.shape[1]
    down = jnp.concatenate([a_query[0].T, a_value[0].T], axis=0)
    full, low_rank, up_query, up_value = project(
        tokens, w_query, w_key, w_value, down, b_query[0], b_value[0],
        block_adapter, adapter_slot, adapter_ranks,
    )
    part, up_q, up_v = attend(
        full, low_rank, up_query, up_value, d_heads,
        block_adapter, adapter_slot, adapter_ranks, live_tokens,
    )
    low, grad_bq, grad_bv = reduce_grads(
        tokens, width, block_adapter, adapter_slot, adapter_ranks, part, up_q, up_v
    )
    return (low[:R].T[None], grad_bq[None], low[R:].T[None], grad_bv[None])


def solution(mesh):
    in_specs = (
        P(("groups", "dp"), None),
        P("dp", "tensor"),
        P("dp", "tensor"),
        P("dp", "tensor"),
        P(("groups", "dp"), "tensor", None),
        P(("groups", "dp"), None, "tensor"),
        P(("groups", "dp"), "tensor", None),
        P(("groups", "dp"), None, "tensor"),
        P("groups"),
        P(),
        P(("groups", "dp"), None),
        P(("groups", "dp")),
        P(("groups", "dp"), "tensor"),
    )
    out_specs = (
        P(("groups", "dp"), "tensor", None),
        P(("groups", "dp"), None, "tensor"),
        P(("groups", "dp"), "tensor", None),
        P(("groups", "dp"), None, "tensor"),
    )
    return jax.shard_map(
        on_device, mesh=mesh, in_specs=in_specs, out_specs=out_specs, check_vma=False
    )
```
